32 devices in a mesh: group: 2 (over y), seq: 4 (over z), tensor: 4 (over x, core).
Axes of the slice: x: 2, y: 2, z: 4, core: 2. Of those that a mesh axis runs over, the one named last changes fastest.
Arguments:
- query: bfloat16 [16, 7168], P(('group', 'seq'), 'tensor'), parts along dimension 0, may hold values from -5 to 5
- key_cache: bfloat16 [32, 256, 7168], P(('group', 'seq'), None, 'tensor'), parts along dimension 0, may hold values from -5 to 5
- value_cache: bfloat16 [32, 256, 7168], P(('group', 'seq'), None, 'tensor'), parts along dimension 0, may hold values from -6 to 6
- alibi_slopes: float32 [56], P('tensor'), may hold values from 0 to 1, as said below
- block_seq: int32 [32], P(('group', 'seq')), parts along dimension 0, may hold values from 0 to 7, as said below
- block_pos: int32 [32], P(('group', 'seq')), parts along dimension 0, may hold values from 0 to 2, as said below
- lengths: int32 [16], P('group'), parts along dimension 0, may hold values from 1 to 768, as said below
- out_weight: bfloat16 [7168, 14336], P('tensor', 'seq'), may hold values from -0.5 to 0.5
Outputs:
- mixed: bfloat16 [16, 14336], P(('group', 'tensor'), 'seq'), parts along dimension 0
The draws below stay inside these ranges and needn't reach their ends.
There are 2 independent parts, one for each index of `group`. The reference program is written for one: setup_inputs(seed, part) draws one part's arguments, and reference() takes and returns one part's arrays. A program takes and returns all parts, laid end to end along the dimension named above; an argument that names none is the same for every part. Nothing has to cross between parts.
Inputs may be any that keep to these rules, and one draw needn't show every extreme that they name: `block_seq`: every sequence owns at least one block and at most 3; the blocks of sequence s have block_pos 0 to n_s - 1, each once. block_pos of a block is below the number of blocks its sequence owns. `lengths`: A sequence that owns n blocks has a length above 256 * (n - 1) and at most 256 * n. `alibi_slopes`: positive slopes.
All inputs are finite; a program needn't handle non-finite values.
Results may differ from the reference program's by a relative error of at most 0.0054.
Values may be sent and summed in bfloat16 or wider, within the bound.
No kernel may reach another device: no remote copies, remote signals or barrier semaphores. Data moves between devices by JAX's collectives and lax.ppermute only.
A program may use at most 64 MiB of HBM per device.

```python
import math
import jax
import jax.numpy as jnp
from jax import lax

D = 14336
HEADS = 56
HEAD_DIM = 128
BLOCK = 256
SEQS = 8
BLOCKS = 16
MOST_BLOCKS = 3


def block_layout(key):
    second = jax.random.fold_in(key, 12)
    third = jax.random.fold_in(key, 13)
    fourth = jax.random.fold_in(key, 14)
    fifth = jax.random.fold_in(key, 15)
    extra = BLOCKS - SEQS
    capacity = MOST_BLOCKS - 1
    remain = extra - capacity
    relabel = jax.random.permutation(third, SEQS).astype(jnp.int32)
    longest = relabel[0]
    seq_ids = jnp.arange(SEQS, dtype=jnp.int32)
    counts = 1 + capacity * (seq_ids == longest).astype(jnp.int32)
    if remain > 0:
        order = jax.random.permutation(second, (SEQS - 1) * capacity)[:remain].astype(jnp.int32)
        target = relabel[1 + order // capacity]
        counts = counts + jnp.sum((target[:, None] == seq_ids[None, :]).astype(jnp.int32), axis=0)
    ends = jnp.cumsum(counts).astype(jnp.int32)
    starts = ends - counts
    slots = jnp.arange(BLOCKS, dtype=jnp.int32)
    seq_of = jnp.sum((ends[None, :] <= slots[:, None]).astype(jnp.int32), axis=1)
    pos_of = slots - starts[seq_of]
    placed = jax.random.permutation(fourth, BLOCKS)
    owners = jnp.zeros((BLOCKS,), jnp.int32).at[placed].set(seq_of)
    places = jnp.zeros((BLOCKS,), jnp.int32).at[placed].set(pos_of)
    tails = jax.random.randint(fifth, (SEQS,), 1, BLOCK + 1).astype(jnp.int32)
    tails = jnp.where(seq_ids == longest, BLOCK, tails)
    sizes_out = ((counts - 1) * BLOCK + tails).astype(jnp.int32)
    return (owners, places, sizes_out)


def draw_block_seq(key, part):
    return block_layout(key)[0]


def draw_block_pos(key, part):
    return block_layout(key)[1]


def draw_lengths(key, part):
    return block_layout(key)[2]


def draw_query(key, part):
    base = jnp.clip(jax.random.normal(jax.random.fold_in(key, 21), (SEQS, HEADS, HEAD_DIM), jnp.float32), -5.0, 5.0)
    return base.reshape(SEQS, HEADS * HEAD_DIM).astype(jnp.bfloat16)


def draw_key_cache(key, part):
    base = jnp.clip(jax.random.normal(jax.random.fold_in(key, 23), (BLOCKS, BLOCK, HEADS * HEAD_DIM), jnp.float32), -5.0, 5.0)
    return base.astype(jnp.bfloat16)


def draw_alibi_slopes(key, part):
    spread = jax.random.uniform(jax.random.fold_in(key, 32), (HEADS,), jnp.float32)
    strong = jax.random.randint(jax.random.fold_in(key, 31), (HEADS,), 0, 2) == 1
    slow = jnp.exp(jnp.log(1.0 / 8192.0) + spread * jnp.log(8.0))
    fast = jnp.exp(jnp.log(1.0 / 64.0) + spread * jnp.log(8.0))
    return jnp.where(strong, fast, slow).astype(jnp.float32)


def steps_of(rng, shape, shards, least, high):
    factor_of, own = 1.0, jax.random.fold_in(rng, 6)
    for axis_at, parts in shards:
        steps = jnp.exp(jax.random.uniform(jax.random.fold_in(own, axis_at), (parts,), jnp.float32, least / len(shards), high / len(shards)))
        factor_of = factor_of * jnp.repeat(steps, shape[axis_at] // parts).reshape([-1 if axis == axis_at else 1 for axis in range(len(shape))])
    return factor_of


def scatter_about(rng, extent, deviation, bound, split=(), kind=jnp.bfloat16):
    array = jax.random.normal(rng, extent, jnp.float32) * deviation
    if len(split) > 0:
        array = steps_of(rng, extent, split, -0.22, 0.18) * array
    return jnp.clip(array, min=-bound, max=bound).astype(kind)


def setup_inputs(seed: int = 0, part: int = 0) -> dict:
    streams_of = jax.random.split(jax.random.key(seed), 9)
    part_keys = jax.random.split(jax.random.fold_in(streams_of[8], part), 9)
    return {
        "query": draw_query(jax.random.fold_in(jax.random.fold_in(streams_of[8], part), 71), part),
        "key_cache": draw_key_cache(jax.random.fold_in(jax.random.fold_in(streams_of[8], part), 71), part),
        "value_cache": scatter_about(part_keys[2], (BLOCKS, BLOCK, HEADS * HEAD_DIM), 1.0, 6.0, ((0, 4), (2, 4))),
        "alibi_slopes": draw_alibi_slopes(jax.random.fold_in(streams_of[8], 71), part),
        "block_seq": draw_block_seq(jax.random.fold_in(jax.random.fold_in(streams_of[8], part), 71), part),
        "block_pos": draw_block_pos(jax.random.fold_in(jax.random.fold_in(streams_of[8], part), 71), part),
        "lengths": draw_lengths(jax.random.fold_in(jax.random.fold_in(streams_of[8], part), 71), part),
        "out_weight": scatter_about(streams_of[7], (HEADS * HEAD_DIM, D), HEAD_DIM ** -0.5, 0.5, ((0, 4), (1, 4))),
    }


def reference(query, key_cache, value_cache, alibi_slopes, block_seq, block_pos, lengths, out_weight):
    scale = 1.0 / math.sqrt(HEAD_DIM)
    offsets = jnp.arange(BLOCK, dtype=jnp.int32)

    def one_block(index):
        owner = block_seq[index]
        length = lengths[owner]
        placed = block_pos[index] * BLOCK + offsets
        live = placed < length
        qrow = query[owner].astype(jnp.float32).reshape(HEADS, HEAD_DIM)
        keys = key_cache[index].astype(jnp.float32).reshape(BLOCK, HEADS, HEAD_DIM)
        values = value_cache[index].astype(jnp.float32).reshape(BLOCK, HEADS, HEAD_DIM)
        scores = jnp.einsum('thd,hd->ht', keys, qrow) * scale
        distance = (length - 1 - placed).astype(jnp.float32)
        scores = scores - alibi_slopes[:, None] * distance[None, :]
        scores = jnp.where(live[None, :], scores, -1e+30)
        top = lax.optimization_barrier(jnp.max(scores, axis=1))
        weights = jnp.where(live[None, :], jnp.exp(scores - top[:, None]), 0.0)
        total = lax.optimization_barrier(jnp.sum(weights, axis=1))
        rounded = lax.optimization_barrier(weights.astype(jnp.bfloat16)).astype(jnp.float32)
        summed = jnp.einsum('ht,thd->hd', rounded, values)
        return (top, total, summed)
    tops, totals, sums = lax.map(one_block, jnp.arange(BLOCKS, dtype=jnp.int32))
    seq_ids = jnp.arange(SEQS, dtype=jnp.int32)
    owned = block_seq[None, :] == seq_ids[:, None]
    seq_max = lax.optimization_barrier(jnp.max(jnp.where(owned[:, :, None], tops[None], -1e+30), axis=1))
    factor = jnp.where(owned[:, :, None], jnp.exp(tops[None] - seq_max[:, None, :]), 0.0)
    seq_sum = lax.optimization_barrier(jnp.sum(factor * totals[None], axis=1))
    seq_acc = jnp.einsum('sbh,bhd->shd', factor, sums, precision=lax.Precision.HIGHEST)
    attention = (seq_acc / seq_sum[:, :, None]).reshape(SEQS, HEADS * HEAD_DIM).astype(jnp.bfloat16)
    return jnp.dot(attention, out_weight, preferred_element_type=jnp.float32).astype(jnp.bfloat16)
```

```python
import math
from functools import partial

import jax
import jax.numpy as jnp
from jax import lax
from jax.experimental import pallas as pl
from jax.experimental.pallas import tpu as pltpu
from jax.sharding import PartitionSpec as P

F32 = jnp.float32
BF16 = jnp.bfloat16
LANES = 128
DEAD = -1e30
DIRECT = 8
VMEM = pl.BlockSpec(memory_space=pltpu.VMEM)
SMEM = pl.BlockSpec(memory_space=pltpu.SMEM)


def params(mib):
    return pltpu.CompilerParams(vmem_limit_bytes=mib << 20)


def from_peers(x, axis):
    size = lax.axis_size(axis)
    if size > DIRECT or size & (size - 1):
        return [lax.all_gather(x, axis, axis=0, tiled=True)]
    return [x] + [swap(x, axis, m) for m in range(1, size)]


def swap(x, axis, m):
    size = lax.axis_size(axis)
    return lax.ppermute(x, axis, [(i, i ^ m) for i in range(size)])


def pad_rows(n):
    return -(-n // 16) * 16


def prep_kernel(slopes, block_seq, block_pos, lengths, bias, pick, owner, *, direct):
    blocks, rows, block_len = bias.shape
    seqs = pick.shape[1]
    here = lax.axis_index("seq") if direct else 0
    per_home = seqs // lax.axis_size("seq")
    head = lax.broadcasted_iota(jnp.int32, (rows, block_len), 0)
    slope = jnp.zeros((rows, block_len), F32)
    for h in range(slopes.shape[0]):
        slope = jnp.where(head == h, slopes[h], slope)
    offset = lax.broadcasted_iota(jnp.int32, (rows, block_len), 1)
    row = lax.broadcasted_iota(jnp.int32, (seqs, LANES), 0)
    for b in range(blocks):
        seq = block_seq[b]
        length = lengths[seq]
        place = block_pos[b] * block_len + offset
        distance = (length - 1 - place).astype(F32)
        bias[b] = jnp.where(place < length, -(slope * distance), DEAD)
        at = ((seq // per_home) ^ here) * per_home + seq % per_home
        pick[b] = jnp.where(row == at, 1.0, 0.0).astype(F32)
        owner[b : b + 1, :] = jnp.full((1, LANES), seq, jnp.int32).astype(F32)


def attend_kernel(bias, pick, owner, keys, values, *rest, scale, heads):
    queries, out, whole = rest[:-2], rest[-2], rest[-1]
    blocks, rows, _ = bias.shape
    features = keys.shape[2]
    size = features // heads
    at = 0
    for part in queries:
        whole[at : at + part.shape[0], :] = part[...].astype(F32)
        at += part.shape[0]
    head = lax.broadcasted_iota(jnp.int32, (rows, size), 0)
    row = lax.broadcasted_iota(jnp.int32, (rows, LANES), 0)
    lane = lax.broadcasted_iota(jnp.int32, (rows, LANES), 1)
    all_rows = whole[...]
    for b in range(blocks):
        mine = pick[b]
        spread = []
        for h in range(heads):
            query = jnp.sum(all_rows[:, h * size : (h + 1) * size] * mine[:, :size], axis=0, keepdims=True)
            spread.append(jnp.where(head == h, query, 0.0))
        query = jnp.concatenate(spread, axis=1).astype(BF16)
        scores = lax.dot_general(query, keys[b], (((1,), (1,)), ((), ())), preferred_element_type=F32)
        scores = scores * scale + bias[b]
        top = jnp.max(scores, axis=1, keepdims=True)
        weights = jnp.exp(scores - top)
        total = jnp.sum(weights, axis=1, keepdims=True)
        sums = jnp.dot(weights.astype(BF16), values[b], preferred_element_type=F32)
        for h in range(heads):
            out[b : b + 1, h * size : (h + 1) * size] = sums[h : h + 1, h * size : (h + 1) * size]
        stats = jnp.where(lane == row, top, 0.0) + jnp.where(lane == row + LANES // 2, total, 0.0)
        out[b : b + 1, features : features + LANES] = jnp.sum(stats, axis=0, keepdims=True)
        out[b : b + 1, features + LANES :] = owner[b : b + 1, :]


def project_kernel(weight, *rest, heads, parts):
    partials, outs, acc = rest[:parts], rest[parts:-1], rest[-1]
    seqs = acc.shape[0]
    features = weight.shape[0]
    size = features // heads
    peers = len(outs)
    each = seqs // peers
    t = lax.axis_index("tensor")
    row = lax.broadcasted_iota(jnp.int32, (seqs, LANES), 0)
    target = (((row // each) ^ t) * each + row % each).astype(F32)

    def stats_of(line):
        mine = line[:, features + LANES :] == target
        stats = jnp.broadcast_to(line[:, features : features + LANES], (seqs, LANES))
        return mine, stats

    def over_blocks(step, carry):
        for ref in partials:
            count = ref.shape[0]
            if count <= 8 or count % 8:
                for b in range(count):
                    carry = step(ref[b : b + 1, :], carry)
            else:

                def eight(g, carry, ref=ref):
                    lines = ref[pl.ds(pl.multiple_of(g * 8, 8), 8), :]
                    for b in range(8):
                        carry = step(lines[b : b + 1], carry)
                    return carry

                carry = lax.fori_loop(0, count // 8, eight, carry)
        return carry

    def highest(line, best):
        mine, stats = stats_of(line)
        return jnp.maximum(best, jnp.where(mine, stats, DEAD))

    best = over_blocks(highest, jnp.full((seqs, LANES), DEAD, F32))

    def add_up(line, carry):
        total, sums = carry
        mine, stats = stats_of(line)
        factor = jnp.where(mine, jnp.exp(stats - best), 0.0)
        total = total + factor * pltpu.roll(stats, LANES // 2, 1)
        new = []
        for h in range(heads):
            value = line[:, h * size : (h + 1) * size]
            new.append(sums[h] + jnp.broadcast_to(factor[:, h : h + 1], (seqs, size)) * value)
        return total, tuple(new)

    zeros = tuple(jnp.zeros((seqs, size), F32) for _ in range(heads))
    total, sums = over_blocks(add_up, (jnp.zeros((seqs, LANES), F32), zeros))
    for h in range(heads):
        acc[:, h * size : (h + 1) * size] = sums[h] / total[:, h : h + 1]
    attention = acc[...].astype(BF16)
    columns = weight.shape[1]
    step = 512 if columns % 512 == 0 else columns
    for c in range(0, columns, step):
        mixed = jnp.dot(attention, weight[:, c : c + step], preferred_element_type=F32)
        for m, out in enumerate(outs):
            out[:, c : c + step] = mixed[m * each : (m + 1) * each]


def local(query, key_cache, value_cache, alibi_slopes, block_seq, block_pos, lengths, out_weight):
    heads = alibi_slopes.shape[0]
    features = query.shape[1]
    blocks, block_len = key_cache.shape[:2]
    seqs = lengths.shape[0]
    columns = out_weight.shape[1]
    peers = lax.axis_size("tensor")
    rows = pad_rows(heads)
    scale = 1.0 / math.sqrt(features // heads)
    keys, values, weight = (
        pltpu.with_memory_space_constraint(a, pltpu.VMEM) for a in (key_cache, value_cache, out_weight)
    )
    queries = from_peers(query, "seq")
    bias, pick, owner = pl.pallas_call(
        partial(prep_kernel, direct=len(queries) > 1),
        out_shape=[
            jax.ShapeDtypeStruct((blocks, rows, block_len), F32),
            jax.ShapeDtypeStruct((blocks, seqs, LANES), F32),
            jax.ShapeDtypeStruct((blocks, LANES), F32),
        ],
        in_specs=[SMEM] * 4,
        out_specs=[VMEM] * 3,
        compiler_params=params(4),
        cost_estimate=pl.CostEstimate(flops=20_000_000_000, transcendentals=0, bytes_accessed=1 << 16),
        name="prep",
    )(alibi_slopes, block_seq, block_pos, lengths)
    partial_rows = pl.pallas_call(
        partial(attend_kernel, scale=scale, heads=heads),
        out_shape=jax.ShapeDtypeStruct((blocks, features + 2 * LANES), F32),
        in_specs=[VMEM] * (5 + len(queries)),
        out_specs=VMEM,
        scratch_shapes=[pltpu.VMEM((seqs, features), F32)],
        compiler_params=params(12),
        name="attend",
    )(bias, pick, owner, keys, values, *queries)
    partials = from_peers(partial_rows, "seq")
    mixed = pl.pallas_call(
        partial(project_kernel, heads=heads, parts=len(partials)),
        out_shape=[jax.ShapeDtypeStruct((seqs // peers, columns), F32)] * peers,
        in_specs=[VMEM] * (1 + len(partials)),
        out_specs=[VMEM] * peers,
        scratch_shapes=[pltpu.VMEM((seqs, features), F32)],
        compiler_params=params(12),
        name="project",
    )(weight, *partials)
    whole = mixed[0]
    for m in range(1, peers):
        whole = whole + swap(mixed[m], "tensor", m)
    return whole.astype(BF16)


def solution(mesh):
    placed = (
        P(("group", "seq"), "tensor"),
        P(("group", "seq"), None, "tensor"),
        P(("group", "seq"), None, "tensor"),
        P("tensor"),
        P(("group", "seq")),
        P(("group", "seq")),
        P("group"),
        P("tensor", "seq"),
    )
    return jax.shard_map(
        local, mesh=mesh, in_specs=placed, out_specs=P(("group", "tensor"), "seq"), check_vma=False
    )
```
